32 devices in a mesh: ep: 8 (over z, y), rep: 4 (over x, core).
Axes of the slice: x: 2, y: 2, z: 4, core: 2. Of those that a mesh axis runs over, the one named last changes fastest.
Arguments:
- tokens: bfloat16 [4096, 2304], P(('ep', 'rep')), may hold values from -6 to 6
- output_grad: bfloat16 [4096, 2304], P(('ep', 'rep')), may hold values from -2 to 2
- chosen_experts: int32 [4096, 8], P(('ep', 'rep')), may hold values from 0 to 31, all different within a row; in each aligned block of 128 rows (0 to 127, 128 to 255, ...) at most 36 rows name the same one
- route_weights: float32 [4096, 8], P(('ep', 'rep')), may hold values from 0.1 to 0.5
- gate_weight: bfloat16 [32, 2304, 1024], P(('ep', 'rep')), may hold values from -0.125 to 0.125
- up_weight: bfloat16 [32, 2304, 1024], P(('ep', 'rep')), may hold values from -0.125 to 0.125
- down_weight: bfloat16 [32, 1024, 2304], P(('ep', 'rep')), may hold values from -0.1875 to 0.1875
- gate_adapter_in: bfloat16 [32, 16, 2304], P(('ep', 'rep')), may hold values from -0.125 to 0.125
- gate_adapter_out: bfloat16 [32, 16, 1024], P(('ep', 'rep')), may hold values from -1 to 1
- up_adapter_in: bfloat16 [32, 16, 2304], P(('ep', 'rep')), may hold values from -0.125 to 0.125
- up_adapter_out: bfloat16 [32, 16, 1024], P(('ep', 'rep')), may hold values from -1 to 1
- shared_gate: bfloat16 [2304, 512], P(None, 'rep'), may hold values from -0.125 to 0.125
- shared_up: bfloat16 [2304, 512], P(None, 'rep'), may hold values from -0.125 to 0.125
- shared_down: bfloat16 [2304, 512], P(None, 'rep'), may hold values from -0.25 to 0.25
Outputs:
- token_grad: bfloat16 [4096, 2304], P(('ep', 'rep'))
- gate_in_grad: float32 [32, 16, 2304], P(('ep', 'rep'))
- gate_out_grad: float32 [32, 16, 1024], P(('ep', 'rep'))
- up_in_grad: float32 [32, 16, 2304], P(('ep', 'rep'))
- up_out_grad: float32 [32, 16, 1024], P(('ep', 'rep'))
The draws below stay inside these ranges and needn't reach their ends.
Inputs may be any that keep to these rules, and one draw needn't show every extreme that they name: `chosen_experts`: each row names 8 different experts. In each aligned block of 128 rows no expert is named by more than 36 rows, and in some block an expert is named by exactly 36 rows.
All inputs are finite; a program needn't handle non-finite values.
Results may differ from the reference program's by a relative error of at most 0.0064.
Values may be sent and summed in bfloat16 or wider, within the bound.
No kernel may reach another device: no remote copies, remote signals or barrier semaphores. Data moves between devices by JAX's collectives and lax.ppermute only.
A program may use at most 128 MiB of HBM per device.

```python
import math
import jax
import jax.numpy as jnp
import numpy as np
from jax import lax

D = 2304
FF = 1024
SFF = 512
RANK = 16
TOP = 8
TOK_DEV = 128
EXPERTS = 32
CAP = 36
TOKENS = 4096
N_EP = 8
N_REP = 4


def block_levels(key, extent, shards, low, largest):
    def one(dim, shards_of):
        steps = jax.random.uniform(jax.random.fold_in(jax.random.fold_in(key, 6), dim), (shards_of,), jnp.float32, low / len(shards), largest / len(shards))
        return jnp.repeat(jnp.exp(steps), extent[dim] // shards_of).reshape((-1,) + (1,) * (len(extent) - dim - 1))

    factor_of = one(*shards[0])
    for cut in shards[1:]:
        factor_of = factor_of * one(*cut)
    return factor_of


def assign_block(stream_key, own, number, rows, count, top, bound, slope):
    order = jax.random.permutation(stream_key, count)
    heavy_load, common = shares(count, rows * top, bound, slope, True), shares(count, rows * top, bound, slope, False)
    places = jnp.arange(count)

    def named(sizes, rotation):
        used = int((sizes > 0).sum())
        fixed = max(1, used // 4)
        moved = fixed + (places - fixed + rotation * (used - fixed)) % max(1, count - fixed)
        return jnp.zeros((count,), jnp.int32).at[order[jnp.where(places < fixed, places, moved)]].set(jnp.asarray(sizes, jnp.int32))

    sizes = jnp.where(number % 4 == 0, named(heavy_load, number // 4), named(common, number - number // 4 - 1))
    mixed = jax.random.permutation(jax.random.fold_in(own, 3), count)
    source_of, receiver = mixed[0:count // 2 * 2:2], mixed[1:count // 2 * 2:2]
    margin = jnp.minimum(sizes[source_of] - 1, bound - sizes[receiver]) // 2
    margin = jnp.where((source_of == order[0]) | (receiver == order[0]) | (sizes[receiver] == 0), 0, jnp.maximum(margin, 0))
    moved = jax.random.randint(jax.random.fold_in(own, 4), (count // 2,), 0, 1 << 20) % (margin + 1)
    sizes = sizes.at[source_of].add(-moved).at[receiver].add(moved)
    items = jnp.searchsorted(jnp.cumsum(sizes), jnp.arange(rows * top), side="right").astype(jnp.int32)
    grid = items.reshape(top, rows).T
    grid = grid[jax.random.permutation(jax.random.fold_in(own, 1), rows)]
    rotation = jax.random.randint(jax.random.fold_in(own, 2), (rows, 1), 0, top)
    return jnp.take_along_axis(grid, (jnp.arange(top)[None, :] + rotation) % top, axis=1)


def shares(number_of, total, bound, slope, full):
    portions = [(1 << 20) // math.isqrt(grade ** slope) + 1 for grade in range(1, number_of + 1)]
    largest = bound if full else min(bound, max(-(-total // number_of), total * portions[0] // sum(portions)))
    least = 1 if total - largest >= number_of - 1 else 0
    given, rest = [largest] + [least] * (number_of - 1), total - largest - least * (number_of - 1)
    while rest > 0:
        movable = [i for i in range(1, number_of) if given[i] < largest] or [i for i in range(1, number_of) if given[i] < bound]
        pool, budget = sum([portions[i] for i in movable]), rest
        for i in movable:
            more = min(bound - given[i], max(1, budget * portions[i] // pool), rest)
            given[i] = given[i] + more
            rest = rest - more
    return np.array(given)


def gaussian(own_key, extent, deviation, most, cuts=(), kind=jnp.bfloat16):
    factor_of = block_levels(own_key, extent, cuts, -0.22, 0.18) if cuts else 1.0
    values = jax.random.normal(own_key, extent, jnp.float32) * deviation * factor_of
    return jnp.minimum(jnp.maximum(values, -most), most).astype(kind)


def setup_inputs(seed: int = 0) -> dict:
    key_of = jax.random.split(jax.random.key(seed), 15)
    tokens = gaussian(key_of[0], (TOKENS, D), 1.0, 6.0, ((0, 32),))
    output_grad = gaussian(key_of[1], (TOKENS, D), 0.3, 2.0, ((0, 32),))
    chosen_experts_keys = jax.random.split(jax.random.fold_in(key_of[2], 1), TOKENS // TOK_DEV)
    chosen_experts_turns = jax.random.permutation(jax.random.fold_in(key_of[2], 3), TOKENS // TOK_DEV)
    chosen_experts = jax.vmap(lambda own, number: assign_block(jax.random.fold_in(key_of[2], 2), own, number, TOK_DEV, EXPERTS, TOP, CAP, 1))(chosen_experts_keys, chosen_experts_turns).reshape((TOKENS, TOP))
    route_weights = jnp.clip(0.1 + 0.4 * jax.random.uniform(key_of[3], (TOKENS, TOP), jnp.float32) ** block_levels(key_of[3], (TOKENS, TOP), ((0, 32),), -0.2, 0.2), 0.1, 0.5)
    gate_weight = gaussian(key_of[4], (EXPERTS, D, FF), D ** -0.5, 0.125, ((0, 32),))
    up_weight = gaussian(key_of[5], (EXPERTS, D, FF), D ** -0.5, 0.125, ((0, 32),))
    down_weight = gaussian(key_of[6], (EXPERTS, FF, D), FF ** -0.5, 0.1875, ((0, 32),))
    gate_adapter_in = gaussian(key_of[7], (EXPERTS, RANK, D), D ** -0.5, 0.125, ((0, 32),))
    gate_adapter_out = gaussian(key_of[8], (EXPERTS, RANK, FF), (2 * RANK) ** -0.5, 1.0, ((0, 32),))
    up_adapter_in = gaussian(key_of[9], (EXPERTS, RANK, D), D ** -0.5, 0.125, ((0, 32),))
    up_adapter_out = gaussian(key_of[10], (EXPERTS, RANK, FF), (2 * RANK) ** -0.5, 1.0, ((0, 32),))
    shared_gate = gaussian(key_of[11], (D, SFF), D ** -0.5, 0.125, ((1, 4),))
    shared_up = gaussian(key_of[12], (D, SFF), D ** -0.5, 0.125, ((1, 4),))
    shared_down = gaussian(key_of[13], (D, SFF), SFF ** -0.5, 0.25, ((1, 4),))
    return dict(tokens=tokens, output_grad=output_grad, chosen_experts=chosen_experts, route_weights=route_weights, gate_weight=gate_weight, up_weight=up_weight, down_weight=down_weight, gate_adapter_in=gate_adapter_in, gate_adapter_out=gate_adapter_out, up_adapter_in=up_adapter_in, up_adapter_out=up_adapter_out, shared_gate=shared_gate, shared_up=shared_up, shared_down=shared_down)


def contract_last(left, right):
    return lax.dot_general(left, right, (((1,), (1,)), ((), ())), preferred_element_type=jnp.float32)


def contract_first(left, right):
    return lax.dot_general(left, right, (((0,), (0,)), ((), ())), preferred_element_type=jnp.float32)


def expert_pass(input_rows, grad_rows, weights):
    gate_w, up_w, down_w, gate_in, gate_out, up_in, up_out = weights
    low_gate = contract_last(input_rows, gate_in).astype(jnp.bfloat16)
    low_up = contract_last(input_rows, up_in).astype(jnp.bfloat16)
    gate_pre = jnp.dot(input_rows, gate_w, preferred_element_type=jnp.float32) + jnp.dot(low_gate, gate_out, preferred_element_type=jnp.float32)
    up_pre = jnp.dot(input_rows, up_w, preferred_element_type=jnp.float32) + jnp.dot(low_up, up_out, preferred_element_type=jnp.float32)
    d_hidden = contract_last(grad_rows, down_w)
    gate_sigmoid = jax.nn.sigmoid(gate_pre)
    d_gate = (d_hidden * up_pre * gate_sigmoid * (1.0 + gate_pre * (1.0 - gate_sigmoid))).astype(jnp.bfloat16)
    d_up = (d_hidden * gate_pre * gate_sigmoid).astype(jnp.bfloat16)
    low_dgate = contract_last(d_gate, gate_out).astype(jnp.bfloat16)
    low_dup = contract_last(d_up, up_out).astype(jnp.bfloat16)
    row_grads = contract_last(d_gate, gate_w) + jnp.dot(low_dgate, gate_in, preferred_element_type=jnp.float32)
    row_grads = row_grads + contract_last(d_up, up_w) + jnp.dot(low_dup, up_in, preferred_element_type=jnp.float32)
    adapter_grads = (contract_first(low_dgate, input_rows), contract_first(low_gate, d_gate), contract_first(low_dup, input_rows), contract_first(low_up, d_up))
    return row_grads.astype(jnp.bfloat16), adapter_grads


def shared_pass(input_rows, grad_rows, gate_w, up_w, down_w):
    gate_pre = jnp.dot(input_rows, gate_w, preferred_element_type=jnp.float32)
    up_pre = jnp.dot(input_rows, up_w, preferred_element_type=jnp.float32)
    d_hidden = jnp.dot(grad_rows, down_w, preferred_element_type=jnp.float32)
    gate_sigmoid = jax.nn.sigmoid(gate_pre)
    d_gate = (d_hidden * up_pre * gate_sigmoid * (1.0 + gate_pre * (1.0 - gate_sigmoid))).astype(jnp.bfloat16)
    d_up = (d_hidden * gate_pre * gate_sigmoid).astype(jnp.bfloat16)
    return contract_last(d_gate, gate_w) + contract_last(d_up, up_w)


def reference(tokens, output_grad, chosen_experts, route_weights, gate_weight, up_weight, down_weight, gate_adapter_in, gate_adapter_out, up_adapter_in, up_adapter_out, shared_gate, shared_up, shared_down):
    pick_total = TOKENS * TOP
    room = N_EP * N_REP * CAP
    flat_experts = chosen_experts.reshape(pick_total)
    onehot = (flat_experts[:, None] == jnp.arange(EXPERTS, dtype=jnp.int32)[None, :]).astype(jnp.int32)
    position = jnp.sum((jnp.cumsum(onehot, axis=0) - onehot) * onehot, axis=1).astype(jnp.int32)
    table = jnp.full((EXPERTS, room), pick_total, jnp.int32).at[flat_experts, position].set(jnp.arange(pick_total, dtype=jnp.int32))
    owner_token = jnp.concatenate([jnp.arange(pick_total, dtype=jnp.int32) // TOP, jnp.full((1,), TOKENS, jnp.int32)])
    padded_tokens = jnp.concatenate([tokens, jnp.zeros((1, D), jnp.bfloat16)])
    padded_grads = jnp.concatenate([output_grad, jnp.zeros((1, D), jnp.bfloat16)])
    padded_weights = jnp.concatenate([route_weights.reshape(pick_total), jnp.zeros((1,), jnp.float32)])

    def expert_step(total, expert):
        pick_rows = table[expert]
        token_index = owner_token[pick_rows]
        input_rows = padded_tokens[token_index]
        grad_rows = (padded_weights[pick_rows][:, None] * padded_grads[token_index].astype(jnp.float32)).astype(jnp.bfloat16)
        weights = (gate_weight[expert], up_weight[expert], down_weight[expert], gate_adapter_in[expert], gate_adapter_out[expert], up_adapter_in[expert], up_adapter_out[expert])
        row_grads, adapter_grads = expert_pass(input_rows, grad_rows, weights)
        total = total.at[token_index].add(row_grads.astype(jnp.float32))
        return total, adapter_grads

    total, adapter_grads = lax.scan(expert_step, jnp.zeros((TOKENS + 1, D), jnp.float32), jnp.arange(EXPERTS, dtype=jnp.int32))
    shared_grad = shared_pass(tokens, output_grad, shared_gate, shared_up, shared_down)
    token_grad = (total[:TOKENS] + shared_grad).astype(jnp.bfloat16)
    return token_grad, adapter_grads[0], adapter_grads[1], adapter_grads[2], adapter_grads[3]
```

```python
import functools

import jax
import jax.numpy as jnp
from jax import lax
from jax.experimental import pallas as pl
from jax.experimental.pallas import tpu as pltpu
from jax.sharding import PartitionSpec as P

AXES = ("ep", "rep")
F32 = jnp.float32
BF16 = jnp.bfloat16


def dot(left, right, left_dim, right_dim):
    return lax.dot_general(
        left, right, (((left_dim,), (right_dim,)), ((), ())), preferred_element_type=F32
    )


def cotangents(gate_pre, up_pre, d_hidden):
    sig = jax.nn.sigmoid(gate_pre)
    d_gate = (d_hidden * up_pre * sig * (1.0 + gate_pre * (1.0 - sig))).astype(BF16)
    d_up = (d_hidden * gate_pre * sig).astype(BF16)
    return d_gate, d_up


def params(mib=56):
    return pltpu.CompilerParams(vmem_limit_bytes=mib * 1024 * 1024)


def selection(info_refs, peers, cap, want_weights):
    count = len(info_refs)
    info = [ref[...] for ref in info_refs]
    tokens = info[0].shape[1]
    places = jnp.concatenate(
        [jnp.where(a[:peers] >= 0.0, a[:peers] + float(i * cap), -1.0) for i, a in enumerate(info)],
        axis=1,
    )
    row = lax.broadcasted_iota(jnp.int32, (count * cap, count * tokens), 0).astype(F32)
    hot = [(row == places[d : d + 1, :]).astype(F32) for d in range(peers)]
    scale = None
    if want_weights:
        weights = jnp.concatenate([a[peers : 2 * peers] for a in info], axis=1)
        scale = jnp.concatenate(
            [
                jnp.sum(hot[d] * weights[d : d + 1, :], axis=1, keepdims=True)
                for d in range(peers)
            ],
            axis=0,
        )
    return jnp.concatenate(hot, axis=0), scale


def pack_kernel(peers, cap, count, scaled, *refs):
    info_refs, block_refs, out_refs = refs[:count], refs[count : 2 * count], refs[2 * count :]
    hot, scale = selection(info_refs, peers, cap, scaled)
    rows = jnp.concatenate([ref[...] for ref in block_refs], axis=0)
    picked = dot(hot.astype(BF16), rows, 1, 0)
    if scaled:
        picked = picked * scale
    for d in range(peers):
        out_refs[d][...] = picked[d * count * cap : (d + 1) * count * cap].astype(BF16)


def pack(infos, blocks, peers, cap, scaled, name):
    count = len(infos)
    tokens, width = blocks[0].shape
    tile = width // 3 if width % 384 == 0 else width
    whole = pl.BlockSpec(infos[0].shape, lambda i: (0, 0))
    part = pl.BlockSpec((tokens, tile), lambda i: (0, i))
    return pl.pallas_call(
        functools.partial(pack_kernel, peers, cap, count, scaled),
        grid=(width // tile,),
        in_specs=[whole] * count + [part] * count,
        out_specs=[pl.BlockSpec((count * cap, tile), lambda i: (0, i))] * peers,
        out_shape=[jax.ShapeDtypeStruct((count * cap, width), BF16)] * peers,
        compiler_params=params(),
        cost_estimate=pl.CostEstimate(
            flops=2 * peers * count * cap * count * tokens * width,
            bytes_accessed=2 * width * (peers * count * cap + count * tokens),
            transcendentals=0,
        ),
        name=name,
    )(*infos, *blocks)


def merge_kernel(peers, cap, count, *refs):
    info_refs, back_refs, out_refs = refs[:count], refs[count : count + peers], refs[count + peers :]
    tokens = info_refs[0].shape[1]
    hot, _ = selection(info_refs, peers, cap, False)
    spread = jnp.transpose(hot).astype(BF16)
    back = jnp.concatenate([ref[...].astype(F32) for ref in back_refs], axis=0).astype(BF16)
    total = dot(spread, back, 1, 0)
    for i in range(count):
        out_refs[i][...] = total[i * tokens : (i + 1) * tokens].astype(out_refs[i].dtype)


def merge(infos, back, peers, cap, kinds, name):
    count = len(infos)
    tokens = infos[0].shape[1]
    width = back[0].shape[1]
    tile = width // 3 if width % 384 == 0 else width
    whole = pl.BlockSpec(infos[0].shape, lambda i: (0, 0))
    return pl.pallas_call(
        functools.partial(merge_kernel, peers, cap, count),
        grid=(width // tile,),
        in_specs=[whole] * count + [pl.BlockSpec((count * cap, tile), lambda i: (0, i))] * peers,
        out_specs=[pl.BlockSpec((tokens, tile), lambda i: (0, i))] * count,
        out_shape=[jax.ShapeDtypeStruct((tokens, width), kind) for kind in kinds],
        compiler_params=params(),
        cost_estimate=pl.CostEstimate(
            flops=2 * peers * count * cap * count * tokens * width,
            bytes_accessed=2 * width * (peers * count * cap + count * tokens),
            transcendentals=0,
        ),
        name=name,
    )(*infos, *back)


def expert_kernel(peers, steps, *refs):
    row_refs, grad_refs = refs[:peers], refs[peers : 2 * peers]
    gate_w, up_w, down_w, gate_in, gate_out, up_in, up_out = refs[2 * peers : 2 * peers + 7]
    out_refs = refs[2 * peers + 7 : 3 * peers + 7]
    gate_in_grad, gate_out_grad, up_in_grad, up_out_grad = refs[3 * peers + 7 : 3 * peers + 11]
    rows, grads, total, low_gate, low_up, back_gate, back_up = refs[3 * peers + 11 :]
    step = pl.program_id(0)
    height = row_refs[0].shape[0]

    @pl.when(step == 0)
    def _():
        rows[...] = jnp.concatenate([r[...].astype(F32) for r in row_refs], axis=0).astype(BF16)
        grads[...] = jnp.concatenate([r[...].astype(F32) for r in grad_refs], axis=0).astype(BF16)
        low_gate[...] = dot(rows[...], gate_in[...], 1, 1).astype(BF16)
        low_up[...] = dot(rows[...], up_in[...], 1, 1).astype(BF16)
        back_gate[...] = jnp.zeros_like(back_gate)
        back_up[...] = jnp.zeros_like(back_up)

    gate_pre = dot(rows[...], gate_w[...], 1, 0) + dot(low_gate[...], gate_out[...], 1, 0)
    up_pre = dot(rows[...], up_w[...], 1, 0) + dot(low_up[...], up_out[...], 1, 0)
    d_hidden = dot(grads[...], down_w[...], 1, 1)
    d_gate, d_up = cotangents(gate_pre, up_pre, d_hidden)
    back_gate[...] += dot(d_gate, gate_out[...], 1, 1)
    back_up[...] += dot(d_up, up_out[...], 1, 1)
    gate_out_grad[...] = dot(low_gate[...], d_gate, 0, 0)
    up_out_grad[...] = dot(low_up[...], d_up, 0, 0)
    part = dot(d_gate, gate_w[...], 1, 1) + dot(d_up, up_w[...], 1, 1)

    @pl.when(step == 0)
    def _():
        total[...] = part

    @pl.when(step > 0)
    def _():
        total[...] += part

    @pl.when(step == steps - 1)
    def _():
        low_dgate = back_gate[...].astype(BF16)
        low_dup = back_up[...].astype(BF16)
        done = total[...] + dot(low_dgate, gate_in[...], 1, 0) + dot(low_dup, up_in[...], 1, 0)
        for d in range(peers):
            out_refs[d][...] = done[d * height : (d + 1) * height].astype(BF16)
        gate_in_grad[...] = dot(low_dgate, rows[...], 0, 0)
        up_in_grad[...] = dot(low_dup, rows[...], 0, 0)


def expert(rows, grads, weights, name):
    peers = len(rows)
    height, width = rows[0].shape
    gate_w, up_w, down_w, gate_in, gate_out, up_in, up_out = weights
    hidden = gate_w.shape[1]
    rank = gate_in.shape[0]
    tile = 256 if hidden % 256 == 0 else hidden
    steps = hidden // tile
    count = peers * height
    block = pl.BlockSpec((height, width), lambda i: (0, 0))
    wide = pl.BlockSpec((width, tile), lambda i: (0, i))
    low_in = pl.BlockSpec((rank, width), lambda i: (0, 0))
    low_out = pl.BlockSpec((rank, tile), lambda i: (0, i))
    return pl.pallas_call(
        functools.partial(expert_kernel, peers, steps),
        grid=(steps,),
        in_specs=[block] * (2 * peers)
        + [wide, wide, pl.BlockSpec((tile, width), lambda i: (i, 0)), low_in, low_out, low_in, low_out],
        out_specs=[block] * peers + [low_in, low_out, low_in, low_out],
        out_shape=[jax.ShapeDtypeStruct((height, width), BF16)] * peers
        + [
            jax.ShapeDtypeStruct((rank, width), F32),
            jax.ShapeDtypeStruct((rank, hidden), F32),
            jax.ShapeDtypeStruct((rank, width), F32),
            jax.ShapeDtypeStruct((rank, hidden), F32),
        ],
        scratch_shapes=[
            pltpu.VMEM((count, width), BF16),
            pltpu.VMEM((count, width), BF16),
            pltpu.VMEM((count, width), F32),
            pltpu.VMEM((count, rank), BF16),
            pltpu.VMEM((count, rank), BF16),
            pltpu.VMEM((count, rank), F32),
            pltpu.VMEM((count, rank), F32),
        ],
        compiler_params=params(60),
        cost_estimate=pl.CostEstimate(
            flops=10 * count * width * hidden,
            bytes_accessed=6 * width * (count + hidden),
            transcendentals=count * hidden,
        ),
        name=name,
    )(*rows, *grads, *weights)


def shared_kernel(slices, *refs):
    rows, grads = refs[0], refs[1]
    gates, ups, downs = (refs[2 + i * slices : 2 + (i + 1) * slices] for i in range(3))
    out = refs[2 + 3 * slices]
    for i in range(slices):
        gate_w, up_w = gates[i][...], ups[i][...]
        gate_pre = dot(rows[...], gate_w, 1, 0)
        up_pre = dot(rows[...], up_w, 1, 0)
        d_hidden = dot(grads[...], downs[i][...], 1, 0)
        d_gate, d_up = cotangents(gate_pre, up_pre, d_hidden)
        part = dot(d_gate, gate_w, 1, 1) + dot(d_up, up_w, 1, 1)
        if i == 0:
            out[...] = part
        else:
            out[...] += part


def shared(rows, grads, gates, ups, downs):
    slices = len(gates)
    hidden = gates[0].shape[1]
    count, width = rows.shape
    return pl.pallas_call(
        functools.partial(shared_kernel, slices),
        out_shape=jax.ShapeDtypeStruct((count, width), F32),
        compiler_params=params(),
        cost_estimate=pl.CostEstimate(
            flops=10 * count * width * hidden * slices,
            bytes_accessed=6 * width * hidden * slices,
            transcendentals=count * hidden * slices,
        ),
        name="shared",
    )(rows, grads, *gates, *ups, *downs)


def local(
    tokens,
    output_grad,
    chosen_experts,
    route_weights,
    gate_weight,
    up_weight,
    down_weight,
    gate_adapter_in,
    gate_adapter_out,
    up_adapter_in,
    up_adapter_out,
    shared_gate,
    shared_up,
    shared_down,
):
    rep_count = lax.axis_size("rep")
    owners = lax.axis_size("ep") * rep_count
    peers = 2 * rep_count
    planes = owners // peers
    token_rows, model_width = tokens.shape
    pick_count = chosen_experts.shape[1]
    cap = token_rows * pick_count * 9 // (8 * owners)
    me = lax.axis_index(AXES)

    def swap(array, plane_step, peer_step, name):
        step = plane_step * peers + peer_step
        if step == 0:
            return array
        with jax.named_scope(name):
            return lax.ppermute(array, AXES, [(i, i ^ step) for i in range(owners)])

    ids = me ^ lax.broadcasted_iota(jnp.int32, (owners, 1, 1), 0)
    named = chosen_experts.T[None] == ids
    weight = jnp.sum(jnp.where(named, route_weights.T[None], 0.0), axis=1)
    picked = jnp.any(named, axis=1)
    earlier = (
        lax.broadcasted_iota(jnp.int32, (token_rows, token_rows), 0)
        < lax.broadcasted_iota(jnp.int32, (token_rows, token_rows), 1)
    ).astype(BF16)
    ahead = jnp.dot(picked.astype(BF16), earlier, preferred_element_type=F32)
    place = jnp.where(picked, ahead, -1.0)
    info = jnp.concatenate(
        [place.reshape(planes, peers, token_rows), weight.reshape(planes, peers, token_rows)], axis=1
    )

    groups = [list(range(0, planes, 2)), list(range(1, planes, 2))]
    infos = {p: swap(info[p], p, 0, f"info{p}") for p in range(planes)}
    token_blocks, grad_blocks = {}, {}
    for g, group in enumerate(groups):
        for p in group:
            token_blocks[p] = swap(tokens, p, 0, f"ztok{p}")
        for p in group:
            grad_blocks[p] = swap(output_grad, p, 0, f"zgrad{p}")

    weights = (
        gate_weight[0],
        up_weight[0],
        down_weight[0],
        gate_adapter_in[0],
        gate_adapter_out[0],
        up_adapter_in[0],
        up_adapter_out[0],
    )
    slices = [[shared_gate], [shared_up], [shared_down]]
    bit = rep_count // 2
    while bit:
        slices = [
            held + [swap(piece, 0, bit, f"slice{bit}") for piece in held] for held in slices
        ]
        bit //= 2

    parts = {}
    adapter = []
    for g, group in enumerate(groups):
        seen = [infos[p] for p in group]
        row_out = pack(seen, [token_blocks[p] for p in group], peers, cap, False, f"packt{g}")
        grad_out = pack(seen, [grad_blocks[p] for p in group], peers, cap, True, f"packg{g}")
        rows = [swap(row_out[d], 0, d, f"tok{g}_{d}") for d in range(peers)]
        grads = [swap(grad_out[d], 0, d, f"grad{g}_{d}") for d in range(peers)]
        result = expert(rows, grads, weights, f"expert{g}")
        adapter.append(result[peers:])
        back = [swap(result[d], 0, d, f"ret{g}_{d}") for d in range(peers)]
        kinds = [F32 if p == 0 else BF16 for p in group]
        merged = merge(seen, back, peers, cap, kinds, f"merge{g}")
        for p, part in zip(group, merged):
            parts[p] = swap(part, p, 0, f"zret{p}")
    total = shared(tokens, output_grad, *slices)
    for p in range(planes):
        total = total + parts[p].astype(F32)
    token_grad = total.astype(BF16)
    adapter_grads = [sum(pieces[1:], pieces[0])[None] for pieces in zip(*adapter)]
    return (token_grad, *adapter_grads)


def solution(mesh):
    row = P(AXES, None)
    block = P(AXES, None, None)
    in_specs = (row,) * 4 + (block,) * 7 + (P(None, "rep"),) * 3
    out_specs = (row,) + (block,) * 4
    return jax.shard_map(local, mesh=mesh, in_specs=in_specs, out_specs=out_specs, check_vma=False)
```

```python
import functools

import jax
import jax.numpy as jnp
from jax import lax
from jax.experimental import pallas as pl
from jax.experimental.pallas import tpu as pltpu
from jax.sharding import PartitionSpec as P


AXES = ("ep", "rep")
F32 = jnp.float32
BF16 = jnp.bfloat16


def dot(left, right, left_dim, right_dim):
    return lax.dot_general(
        left, right, (((left_dim,), (right_dim,)), ((), ())), preferred_element_type=F32
    )


def cotangents(gate_pre, up_pre, d_hidden):
    sig = jax.nn.sigmoid(gate_pre)
    d_gate = (d_hidden * up_pre * sig * (1.0 + gate_pre * (1.0 - sig))).astype(BF16)
    d_up = (d_hidden * gate_pre * sig).astype(BF16)
    return d_gate, d_up


def params(mib=56):
    return pltpu.CompilerParams(vmem_limit_bytes=mib * 1024 * 1024)


def selection(info_refs, peers, cap, want_weights):
    count = len(info_refs)
    info = [ref[...] for ref in info_refs]
    tokens = info[0].shape[1]
    places = jnp.concatenate(
        [jnp.where(a[:peers] >= 0.0, a[:peers] + float(i * cap), -1.0) for i, a in enumerate(info)],
        axis=1,
    )
    row = lax.broadcasted_iota(jnp.int32, (count * cap, count * tokens), 0).astype(F32)
    hot = [(row == places[d : d + 1, :]).astype(F32) for d in range(peers)]
    scale = None
    if want_weights:
        weights = jnp.concatenate([a[peers : 2 * peers] for a in info], axis=1)
        scale = jnp.concatenate(
            [
                jnp.sum(hot[d] * weights[d : d + 1, :], axis=1, keepdims=True)
                for d in range(peers)
            ],
            axis=0,
        )
    return jnp.concatenate(hot, axis=0), scale


def pack_kernel(peers, cap, count, scaled, *refs):
    info_refs, block_refs, out_refs = refs[:count], refs[count : 2 * count], refs[2 * count :]
    hot, scale = selection(info_refs, peers, cap, scaled)
    rows = jnp.concatenate([ref[...] for ref in block_refs], axis=0)
    picked = dot(hot.astype(BF16), rows, 1, 0)
    if scaled:
        picked = picked * scale
    for d in range(peers):
        out_refs[d][...] = picked[d * count * cap : (d + 1) * count * cap].astype(BF16)


def pack(infos, blocks, peers, cap, scaled):
    count = len(infos)
    tokens, width = blocks[0].shape
    tile = width // 3 if width % 384 == 0 else width
    whole = pl.BlockSpec(infos[0].shape, lambda i: (0, 0))
    part = pl.BlockSpec((tokens, tile), lambda i: (0, i))
    return pl.pallas_call(
        functools.partial(pack_kernel, peers, cap, count, scaled),
        grid=(width // tile,),
        in_specs=[whole] * count + [part] * count,
        out_specs=[pl.BlockSpec((count * cap, tile), lambda i: (0, i))] * peers,
        out_shape=[jax.ShapeDtypeStruct((count * cap, width), BF16)] * peers,
        compiler_params=params(),
        cost_estimate=pl.CostEstimate(
            flops=2 * peers * count * cap * count * tokens * width,
            bytes_accessed=2 * width * (peers * count * cap + count * tokens),
            transcendentals=0,
        ),
    )(*infos, *blocks)


def merge_kernel(peers, cap, count, *refs):
    info_refs, back_refs, out_refs = refs[:count], refs[count : count + peers], refs[count + peers :]
    tokens = info_refs[0].shape[1]
    hot, _ = selection(info_refs, peers, cap, False)
    spread = jnp.transpose(hot).astype(BF16)
    back = jnp.concatenate([ref[...].astype(F32) for ref in back_refs], axis=0).astype(BF16)
    total = dot(spread, back, 1, 0)
    for i in range(count):
        out_refs[i][...] = total[i * tokens : (i + 1) * tokens].astype(out_refs[i].dtype)


def merge(infos, back, peers, cap, kinds):
    count = len(infos)
    tokens = infos[0].shape[1]
    width = back[0].shape[1]
    tile = width // 3 if width % 384 == 0 else width
    whole = pl.BlockSpec(infos[0].shape, lambda i: (0, 0))
    return pl.pallas_call(
        functools.partial(merge_kernel, peers, cap, count),
        grid=(width // tile,),
        in_specs=[whole] * count + [pl.BlockSpec((count * cap, tile), lambda i: (0, i))] * peers,
        out_specs=[pl.BlockSpec((tokens, tile), lambda i: (0, i))] * count,
        out_shape=[jax.ShapeDtypeStruct((tokens, width), kind) for kind in kinds],
        compiler_params=params(),
        cost_estimate=pl.CostEstimate(
            flops=2 * peers * count * cap * count * tokens * width,
            bytes_accessed=2 * width * (peers * count * cap + count * tokens),
            transcendentals=0,
        ),
    )(*infos, *back)


def expert_kernel(peers, steps, *refs):
    row_refs, grad_refs = refs[:peers], refs[peers : 2 * peers]
    gate_w, up_w, down_w, gate_in, gate_out, up_in, up_out = refs[2 * peers : 2 * peers + 7]
    out_refs = refs[2 * peers + 7 : 3 * peers + 7]
    gate_in_grad, gate_out_grad, up_in_grad, up_out_grad = refs[3 * peers + 7 : 3 * peers + 11]
    rows, grads, total, low_gate, low_up, back_gate, back_up = refs[3 * peers + 11 :]
    step = pl.program_id(0)
    height = row_refs[0].shape[0]

    @pl.when(step == 0)
    def _():
        rows[...] = jnp.concatenate([r[...].astype(F32) for r in row_refs], axis=0).astype(BF16)
        grads[...] = jnp.concatenate([r[...].astype(F32) for r in grad_refs], axis=0).astype(BF16)
        low_gate[...] = dot(rows[...], gate_in[...], 1, 1).astype(BF16)
        low_up[...] = dot(rows[...], up_in[...], 1, 1).astype(BF16)
        back_gate[...] = jnp.zeros_like(back_gate)
        back_up[...] = jnp.zeros_like(back_up)

    gate_pre = dot(rows[...], gate_w[...], 1, 0) + dot(low_gate[...], gate_out[...], 1, 0)
    up_pre = dot(rows[...], up_w[...], 1, 0) + dot(low_up[...], up_out[...], 1, 0)
    d_hidden = dot(grads[...], down_w[...], 1, 1)
    d_gate, d_up = cotangents(gate_pre, up_pre, d_hidden)
    back_gate[...] += dot(d_gate, gate_out[...], 1, 1)
    back_up[...] += dot(d_up, up_out[...], 1, 1)
    gate_out_grad[...] = dot(low_gate[...], d_gate, 0, 0)
    up_out_grad[...] = dot(low_up[...], d_up, 0, 0)
    part = dot(d_gate, gate_w[...], 1, 1) + dot(d_up, up_w[...], 1, 1)

    @pl.when(step == 0)
    def _():
        total[...] = part

    @pl.when(step > 0)
    def _():
        total[...] += part

    @pl.when(step == steps - 1)
    def _():
        low_dgate = back_gate[...].astype(BF16)
        low_dup = back_up[...].astype(BF16)
        done = total[...] + dot(low_dgate, gate_in[...], 1, 0) + dot(low_dup, up_in[...], 1, 0)
        for d in range(peers):
            out_refs[d][...] = done[d * height : (d + 1) * height].astype(BF16)
        gate_in_grad[...] = dot(low_dgate, rows[...], 0, 0)
        up_in_grad[...] = dot(low_dup, rows[...], 0, 0)


def expert(rows, grads, weights):
    peers = len(rows)
    height, width = rows[0].shape
    gate_w, _, _, gate_in, _, _, _ = weights
    hidden = gate_w.shape[1]
    rank = gate_in.shape[0]
    tile = 256 if hidden % 256 == 0 else hidden
    steps = hidden // tile
    count = peers * height
    block = pl.BlockSpec((height, width), lambda i: (0, 0))
    wide = pl.BlockSpec((width, tile), lambda i: (0, i))
    low_in = pl.BlockSpec((rank, width), lambda i: (0, 0))
    low_out = pl.BlockSpec((rank, tile), lambda i: (0, i))
    return pl.pallas_call(
        functools.partial(expert_kernel, peers, steps),
        grid=(steps,),
        in_specs=[block] * (2 * peers)
        + [wide, wide, pl.BlockSpec((tile, width), lambda i: (i, 0)), low_in, low_out, low_in, low_out],
        out_specs=[block] * peers + [low_in, low_out, low_in, low_out],
        out_shape=[jax.ShapeDtypeStruct((height, width), BF16)] * peers
        + [
            jax.ShapeDtypeStruct((rank, width), F32),
            jax.ShapeDtypeStruct((rank, hidden), F32),
            jax.ShapeDtypeStruct((rank, width), F32),
            jax.ShapeDtypeStruct((rank, hidden), F32),
        ],
        scratch_shapes=[
            pltpu.VMEM((count, width), BF16),
            pltpu.VMEM((count, width), BF16),
            pltpu.VMEM((count, width), F32),
            pltpu.VMEM((count, rank), BF16),
            pltpu.VMEM((count, rank), BF16),
            pltpu.VMEM((count, rank), F32),
            pltpu.VMEM((count, rank), F32),
        ],
        compiler_params=params(60),
        cost_estimate=pl.CostEstimate(
            flops=10 * count * width * hidden,
            bytes_accessed=6 * width * (count + hidden),
            transcendentals=count * hidden,
        ),
    )(*rows, *grads, *weights)


def shared_kernel(slices, *refs):
    rows, grads = refs[0], refs[1]
    gates, ups, downs = (refs[2 + i * slices : 2 + (i + 1) * slices] for i in range(3))
    out = refs[2 + 3 * slices]
    for i in range(slices):
        gate_w, up_w = gates[i][...], ups[i][...]
        gate_pre = dot(rows[...], gate_w, 1, 0)
        up_pre = dot(rows[...], up_w, 1, 0)
        d_hidden = dot(grads[...], downs[i][...], 1, 0)
        d_gate, d_up = cotangents(gate_pre, up_pre, d_hidden)
        part = dot(d_gate, gate_w, 1, 1) + dot(d_up, up_w, 1, 1)
        if i == 0:
            out[...] = part
        else:
            out[...] += part


def shared(rows, grads, gates, ups, downs):
    slices = len(gates)
    hidden = gates[0].shape[1]
    count, width = rows.shape
    return pl.pallas_call(
        functools.partial(shared_kernel, slices),
        out_shape=jax.ShapeDtypeStruct((count, width), F32),
        compiler_params=params(),
        cost_estimate=pl.CostEstimate(
            flops=10 * count * width * hidden * slices,
            bytes_accessed=6 * width * hidden * slices,
            transcendentals=count * hidden * slices,
        ),
        name="shared",
    )(rows, grads, *gates, *ups, *downs)


def halvings(count):
    bits = []
    while count > 1:
        count //= 2
        bits.append(count)
    return bits


def plane_groups(planes):
    return [list(range(0, planes, 2)), list(range(1, planes, 2))]


def local(
    tokens,
    output_grad,
    chosen_experts,
    route_weights,
    gate_weight,
    up_weight,
    down_weight,
    gate_adapter_in,
    gate_adapter_out,
    up_adapter_in,
    up_adapter_out,
    shared_gate,
    shared_up,
    shared_down,
):
    rep_count = lax.axis_size("rep")
    owners = lax.axis_size("ep") * rep_count
    peers = 2 * rep_count
    planes = owners // peers
    token_rows, _ = tokens.shape
    pick_count = chosen_experts.shape[1]
    cap = token_rows * pick_count * 9 // (8 * owners)
    me = lax.axis_index(AXES)

    def swap(array, plane_step, peer_step):
        step = plane_step * peers + peer_step
        if step == 0:
            return array
        return lax.ppermute(array, AXES, [(i, i ^ step) for i in range(owners)])

    ids = me ^ lax.broadcasted_iota(jnp.int32, (owners, 1, 1), 0)
    named = chosen_experts.T[None] == ids
    weight = jnp.sum(jnp.where(named, route_weights.T[None], 0.0), axis=1)
    picked = jnp.any(named, axis=1)
    earlier = (
        lax.broadcasted_iota(jnp.int32, (token_rows, token_rows), 0)
        < lax.broadcasted_iota(jnp.int32, (token_rows, token_rows), 1)
    ).astype(BF16)
    ahead = jnp.dot(picked.astype(BF16), earlier, preferred_element_type=F32)
    place = jnp.where(picked, ahead, -1.0)
    info = jnp.concatenate(
        [place.reshape(planes, peers, token_rows), weight.reshape(planes, peers, token_rows)], axis=1
    )

    groups = plane_groups(planes)
    infos = {p: swap(info[p], p, 0) for p in range(planes)}
    token_blocks, grad_blocks = {}, {}
    for group in groups:
        for p in group:
            token_blocks[p] = swap(tokens, p, 0)
        for p in group:
            grad_blocks[p] = swap(output_grad, p, 0)

    weights = (
        gate_weight[0],
        up_weight[0],
        down_weight[0],
        gate_adapter_in[0],
        gate_adapter_out[0],
        up_adapter_in[0],
        up_adapter_out[0],
    )
    slices = {"gate": [shared_gate], "up": [shared_up], "down": [shared_down]}
    for bit in halvings(rep_count):
        for kind, held in slices.items():
            slices[kind] = held + [swap(piece, 0, bit) for piece in held]

    parts = {}
    adapter = []
    for group in groups:
        seen = [infos[p] for p in group]
        row_out = pack(seen, [token_blocks[p] for p in group], peers, cap, False)
        grad_out = pack(seen, [grad_blocks[p] for p in group], peers, cap, True)
        rows = [swap(row_out[d], 0, d) for d in range(peers)]
        grads = [swap(grad_out[d], 0, d) for d in range(peers)]
        result = expert(rows, grads, weights)
        adapter.append(result[peers:])
        back = [swap(result[d], 0, d) for d in range(peers)]
        kinds = [F32 if p == 0 else BF16 for p in group]
        merged = merge(seen, back, peers, cap, kinds)
        for p, part in zip(group, merged):
            parts[p] = swap(part, p, 0)
    total = shared(tokens, output_grad, *slices.values())
    for p in range(planes):
        total = total + parts[p].astype(F32)
    token_grad = total.astype(BF16)
    adapter_grads = [sum(pieces[1:], pieces[0])[None] for pieces in zip(*adapter)]
    return (token_grad, *adapter_grads)


def solution(mesh):
    row = P(AXES, None)
    block = P(AXES, None, None)
    in_specs = (row,) * 4 + (block,) * 7 + (P(None, "rep"),) * 3
    out_specs = (row,) + (block,) * 4

    return jax.shard_map(local, mesh=mesh, in_specs=in_specs, out_specs=out_specs, check_vma=False)
```

```python
import functools

import jax
import jax.numpy as jnp
from jax import lax
from jax.experimental import pallas as pl
from jax.experimental.pallas import tpu as pltpu
from jax.sharding import PartitionSpec as P


AXES = ("ep", "rep")
F32 = jnp.float32
BF16 = jnp.bfloat16


def dot(left, right, left_dim, right_dim):
    return lax.dot_general(
        left, right, (((left_dim,), (right_dim,)), ((), ())), preferred_element_type=F32
    )


def cotangents(gate_pre, up_pre, d_hidden):
    sig = jax.nn.sigmoid(gate_pre)
    d_gate = (d_hidden * up_pre * sig * (1.0 + gate_pre * (1.0 - sig))).astype(BF16)
    d_up = (d_hidden * gate_pre * sig).astype(BF16)
    return d_gate, d_up


def params(mib=56):
    return pltpu.CompilerParams(vmem_limit_bytes=mib * 1024 * 1024)


def selection(info_refs, peers, cap, want_weights):
    count = len(info_refs)
    info = [ref[...] for ref in info_refs]
    tokens = info[0].shape[1]
    places = jnp.concatenate(
        [jnp.where(a[:peers] >= 0.0, a[:peers] + float(i * cap), -1.0) for i, a in enumerate(info)],
        axis=1,
    )
    row = lax.broadcasted_iota(jnp.int32, (count * cap, count * tokens), 0).astype(F32)
    hot = [(row == places[d : d + 1, :]).astype(F32) for d in range(peers)]
    scale = None
    if want_weights:
        weights = jnp.concatenate([a[peers : 2 * peers] for a in info], axis=1)
        scale = jnp.concatenate(
            [
                jnp.sum(hot[d] * weights[d : d + 1, :], axis=1, keepdims=True)
                for d in range(peers)
            ],
            axis=0,
        )
    return jnp.concatenate(hot, axis=0), scale


def tile_of(width):
    return 768 if width % 768 == 0 else width


def pack_kernel(peers, cap, count, scaled, *refs):
    info_refs, block_refs, out_refs = refs[:count], refs[count : 2 * count], refs[2 * count :]
    hot, scale = selection(info_refs, peers, cap, scaled)
    rows = jnp.concatenate([ref[...] for ref in block_refs], axis=0)
    picked = dot(hot.astype(BF16), rows, 1, 0)
    if scaled:
        picked = picked * scale
    for d in range(peers):
        out_refs[d][...] = picked[d * count * cap : (d + 1) * count * cap].astype(BF16)


def pack(infos, blocks, peers, cap, scaled):
    count = len(infos)
    tokens = infos[0].shape[1]
    width = min(array.shape[1] for array, _ in blocks)
    tile = tile_of(width)
    whole = pl.BlockSpec(infos[0].shape, lambda i: (0, 0))
    parts = [
        pl.BlockSpec((tokens, tile), functools.partial(lambda at, i: (0, i + at), start // tile))
        for _, start in blocks
    ]
    return pl.pallas_call(
        functools.partial(pack_kernel, peers, cap, count, scaled),
        grid=(width // tile,),
        in_specs=[whole] * count + parts,
        out_specs=[pl.BlockSpec((count * cap, tile), lambda i: (0, i))] * peers,
        out_shape=[jax.ShapeDtypeStruct((count * cap, width), BF16)] * peers,
        compiler_params=params(),
        cost_estimate=pl.CostEstimate(
            flops=2 * peers * count * cap * count * tokens * width,
            bytes_accessed=2 * width * (peers * count * cap + count * tokens),
            transcendentals=0,
        ),
    )(*infos, *[array for array, _ in blocks])


def merge_kernel(peers, cap, count, *refs):
    info_refs, back_refs, out_refs = refs[:count], refs[count : count + peers], refs[count + peers :]
    tokens = info_refs[0].shape[1]
    hot, _ = selection(info_refs, peers, cap, False)
    spread = jnp.transpose(hot).astype(BF16)
    back = jnp.concatenate([ref[...].astype(F32) for ref in back_refs], axis=0).astype(BF16)
    total = dot(spread, back, 1, 0)
    for i in range(count):
        out_refs[i][...] = total[i * tokens : (i + 1) * tokens].astype(out_refs[i].dtype)


def merge(infos, back, peers, cap, kinds):
    count = len(infos)
    tokens = infos[0].shape[1]
    width = back[0].shape[1]
    tile = tile_of(width)
    whole = pl.BlockSpec(infos[0].shape, lambda i: (0, 0))
    return pl.pallas_call(
        functools.partial(merge_kernel, peers, cap, count),
        grid=(width // tile,),
        in_specs=[whole] * count + [pl.BlockSpec((count * cap, tile), lambda i: (0, i))] * peers,
        out_specs=[pl.BlockSpec((tokens, tile), lambda i: (0, i))] * count,
        out_shape=[jax.ShapeDtypeStruct((tokens, width), kind) for kind in kinds],
        compiler_params=params(),
        cost_estimate=pl.CostEstimate(
            flops=2 * peers * count * cap * count * tokens * width,
            bytes_accessed=2 * width * (peers * count * cap + count * tokens),
            transcendentals=0,
        ),
    )(*infos, *back)


def expert_kernel(peers, steps, pieces, *refs):
    refs = list(refs)

    def take(count):
        taken, refs[:count] = refs[:count], []
        return taken

    row_refs, grad_refs = ([take(peers) for _ in range(n)] for n in pieces[:2])
    gate_w, up_w, down_w, gate_in, gate_out, up_in, up_out = take(7)
    out_refs = [take(peers) for _ in range(pieces[2])]
    gate_in_grad, gate_out_grad, up_in_grad, up_out_grad = take(4)
    rows, grads, total, low, maps_in, back = refs
    step = pl.program_id(0)
    height = row_refs[0][0].shape[0]
    rank = gate_in.shape[0]

    def gather(target, groups):
        at = 0
        for group in groups:
            wide = group[0].shape[1]
            target[:, at : at + wide] = jnp.concatenate(
                [r[...].astype(F32) for r in group], axis=0
            ).astype(BF16)
            at += wide

    @pl.when(step == 0)
    def _():
        gather(rows, row_refs)
        gather(grads, grad_refs)
        maps_in[:rank] = gate_in[...]
        maps_in[rank:] = up_in[...]
        low[...] = dot(rows[...], maps_in[...], 1, 1).astype(BF16)
        back[...] = jnp.zeros_like(back)

    low_gate, low_up = low[:, :rank], low[:, rank:]
    gate_pre = dot(rows[...], gate_w[...], 1, 0) + dot(low_gate, gate_out[...], 1, 0)
    up_pre = dot(rows[...], up_w[...], 1, 0) + dot(low_up, up_out[...], 1, 0)
    d_hidden = dot(grads[...], down_w[...], 1, 1)
    d_gate, d_up = cotangents(gate_pre, up_pre, d_hidden)
    back[:, :rank] += dot(d_gate, gate_out[...], 1, 1)
    back[:, rank:] += dot(d_up, up_out[...], 1, 1)
    gate_out_grad[...] = dot(low_gate, d_gate, 0, 0)
    up_out_grad[...] = dot(low_up, d_up, 0, 0)
    part = dot(d_gate, gate_w[...], 1, 1) + dot(d_up, up_w[...], 1, 1)

    @pl.when(step == 0)
    def _():
        total[...] = part

    @pl.when(step > 0)
    def _():
        total[...] += part

    @pl.when(step == steps - 1)
    def _():
        low_back = back[...].astype(BF16)
        done = total[...] + dot(low_back, maps_in[...], 1, 0)
        at = 0
        for group in out_refs:
            wide = group[0].shape[1]
            for d in range(peers):
                group[d][...] = done[d * height : (d + 1) * height, at : at + wide].astype(BF16)
            at += wide
        in_grads = dot(low_back, rows[...], 0, 0)
        gate_in_grad[...] = in_grads[:rank]
        up_in_grad[...] = in_grads[rank:]


def expert(rows, grads, weights, out_widths):
    peers = len(rows[0])
    height = rows[0][0].shape[0]
    gate_w, _, _, gate_in, _, _, _ = weights
    width, hidden = gate_w.shape
    rank = gate_in.shape[0]
    tile = 512 if hidden % 512 == 0 else hidden
    steps = hidden // tile
    count = peers * height

    def block(wide):
        return pl.BlockSpec((height, wide), lambda i: (0, 0))

    inputs = [array for group in rows + grads for array in group]
    wide = pl.BlockSpec((width, tile), lambda i: (0, i))
    low_in = pl.BlockSpec((rank, width), lambda i: (0, 0))
    low_out = pl.BlockSpec((rank, tile), lambda i: (0, i))
    result = pl.pallas_call(
        functools.partial(expert_kernel, peers, steps, (len(rows), len(grads), len(out_widths))),
        grid=(steps,),
        in_specs=[block(array.shape[1]) for array in inputs]
        + [wide, wide, pl.BlockSpec((tile, width), lambda i: (i, 0)), low_in, low_out, low_in, low_out],
        out_specs=[block(w) for w in out_widths for _ in range(peers)]
        + [low_in, low_out, low_in, low_out],
        out_shape=[jax.ShapeDtypeStruct((height, w), BF16) for w in out_widths for _ in range(peers)]
        + [
            jax.ShapeDtypeStruct((rank, width), F32),
            jax.ShapeDtypeStruct((rank, hidden), F32),
            jax.ShapeDtypeStruct((rank, width), F32),
            jax.ShapeDtypeStruct((rank, hidden), F32),
        ],
        scratch_shapes=[
            pltpu.VMEM((count, width), BF16),
            pltpu.VMEM((count, width), BF16),
            pltpu.VMEM((count, width), F32),
            pltpu.VMEM((count, 2 * rank), BF16),
            pltpu.VMEM((2 * rank, width), BF16),
            pltpu.VMEM((count, 2 * rank), F32),
        ],
        compiler_params=params(60),
        cost_estimate=pl.CostEstimate(
            flops=10 * count * width * hidden,
            bytes_accessed=6 * width * (count + hidden),
            transcendentals=count * hidden,
        ),
    )(*inputs, *weights)
    outs = [result[i * peers : (i + 1) * peers] for i in range(len(out_widths))]
    return outs, result[-4:]


def finish(base, terms):
    def kernel(*refs):
        base_ref, out = refs[0], refs[-1]
        at = 1
        pieces = []
        for term in terms:
            start = 0
            for piece in term:
                pieces.append((start, start + piece.shape[1], refs[at]))
                start += piece.shape[1]
                at += 1
        edges = sorted({0} | {hi for _, hi, _ in pieces})
        for lo, hi in zip(edges, edges[1:]):
            value = base_ref[:, lo:hi]
            for start, stop, ref in pieces:
                if start <= lo and hi <= stop:
                    value = value + ref[:, lo - start : hi - start].astype(F32)
            out[:, lo:hi] = value.astype(BF16)

    flat = [piece for term in terms for piece in term]
    return pl.pallas_call(
        kernel,
        out_shape=jax.ShapeDtypeStruct(base.shape, BF16),
        compiler_params=params(),
        cost_estimate=pl.CostEstimate(
            flops=base.size * (len(terms) + 1),
            bytes_accessed=base.size * (6 + 2 * len(terms)),
            transcendentals=0,
        ),
        name="finish",
    )(base, *flat)


def shared_kernel(slices, *refs):
    rows, grads = refs[0], refs[1]
    gates, ups, downs = (refs[2 + i * slices : 2 + (i + 1) * slices] for i in range(3))
    out = refs[2 + 3 * slices]
    for i in range(slices):
        gate_w, up_w = gates[i][...], ups[i][...]
        gate_pre = dot(rows[...], gate_w, 1, 0)
        up_pre = dot(rows[...], up_w, 1, 0)
        d_hidden = dot(grads[...], downs[i][...], 1, 0)
        d_gate, d_up = cotangents(gate_pre, up_pre, d_hidden)
        part = dot(d_gate, gate_w, 1, 1) + dot(d_up, up_w, 1, 1)
        if i == 0:
            out[...] = part
        else:
            out[...] += part


def shared(rows, grads, gates, ups, downs):
    slices = len(gates)
    hidden = gates[0].shape[1]
    count, width = rows.shape
    return pl.pallas_call(
        functools.partial(shared_kernel, slices),
        out_shape=jax.ShapeDtypeStruct((count, width), F32),
        compiler_params=params(),
        cost_estimate=pl.CostEstimate(
            flops=10 * count * width * hidden * slices,
            bytes_accessed=6 * width * hidden * slices,
            transcendentals=count * hidden * slices,
        ),
        name="shared",
    )(rows, grads, *gates, *ups, *downs)


def halvings(count):
    bits = []
    while count > 1:
        count //= 2
        bits.append(count)
    return bits


def plane_groups(planes):
    return [list(range(0, planes, 2)), list(range(1, planes, 2))]


def widths(width, pieces):
    return [width // pieces] * pieces if width % (768 * pieces) == 0 else [width]


IN_PIECES = 3
OUT_PIECES = 3


def local(
    tokens,
    output_grad,
    chosen_experts,
    route_weights,
    gate_weight,
    up_weight,
    down_weight,
    gate_adapter_in,
    gate_adapter_out,
    up_adapter_in,
    up_adapter_out,
    shared_gate,
    shared_up,
    shared_down,
):
    rep_count = lax.axis_size("rep")
    owners = lax.axis_size("ep") * rep_count
    peers = 2 * rep_count
    planes = owners // peers
    token_rows, model_width = tokens.shape
    pick_count = chosen_experts.shape[1]
    cap = token_rows * pick_count * 9 // (8 * owners)
    me = lax.axis_index(AXES)

    def swap(array, plane_step, peer_step):
        step = plane_step * peers + peer_step
        if step == 0:
            return array
        return lax.ppermute(array, AXES, [(i, i ^ step) for i in range(owners)])

    ids = me ^ lax.broadcasted_iota(jnp.int32, (owners, 1, 1), 0)
    named = chosen_experts.T[None] == ids
    weight = jnp.sum(jnp.where(named, route_weights.T[None], 0.0), axis=1)
    picked = jnp.any(named, axis=1)
    earlier = (
        lax.broadcasted_iota(jnp.int32, (token_rows, token_rows), 0)
        < lax.broadcasted_iota(jnp.int32, (token_rows, token_rows), 1)
    ).astype(BF16)
    ahead = jnp.dot(picked.astype(BF16), earlier, preferred_element_type=F32)
    place = jnp.where(picked, ahead, -1.0)
    info = jnp.concatenate(
        [place.reshape(planes, peers, token_rows), weight.reshape(planes, peers, token_rows)], axis=1
    )

    groups = plane_groups(planes)
    infos = {p: swap(info[p], p, 0) for p in range(planes)}
    every = [model_width]
    in_widths = widths(model_width, IN_PIECES)
    out_widths = widths(model_width, OUT_PIECES)

    weights = (
        gate_weight[0],
        up_weight[0],
        down_weight[0],
        gate_adapter_in[0],
        gate_adapter_out[0],
        up_adapter_in[0],
        up_adapter_out[0],
    )
    slices = {"gate": [shared_gate], "up": [shared_up], "down": [shared_down]}
    for bit in halvings(rep_count):
        for kind, held in slices.items():
            slices[kind] = held + [swap(piece, 0, bit) for piece in held]

    def pieces(array, p, sizes):
        if p == 0:
            return [(array, sum(sizes[:c])) for c in range(len(sizes))]
        found = []
        for c, size in enumerate(sizes):
            start = sum(sizes[:c])
            found.append((swap(array[:, start : start + size], p, 0), 0))
        return found

    def fan_out(arrays):
        return [swap(arrays[d], 0, d) for d in range(peers)]

    terms = []
    adapter = []
    for g, group in enumerate(groups):
        seen = [infos[p] for p in group]
        sizes, out_sizes = (in_widths, every) if g == 0 else (every, out_widths)
        blocks = [pieces(tokens, p, sizes) for p in group]
        rows = []
        for c in range(len(sizes)):
            packed = pack(seen, [block[c] for block in blocks], peers, cap, False)
            rows.append(fan_out(packed))
        blocks = [pieces(output_grad, p, every) for p in group]
        packed = pack(seen, [block[0] for block in blocks], peers, cap, True)
        grads = [fan_out(packed)]
        outs, grads_of_maps = expert(rows, grads, weights, out_sizes)
        adapter.append(grads_of_maps)
        found = {p: [] for p in group}
        for out in outs:
            back = fan_out(out)
            kinds = [F32 if p == 0 else BF16 for p in group]
            merged = merge(seen, back, peers, cap, kinds)
            for p, part in zip(group, merged):
                found[p].append(swap(part, p, 0))
        terms += list(found.values())
    base = shared(tokens, output_grad, *slices.values())
    token_grad = finish(base, terms)
    adapter_grads = [sum(pieces[1:], pieces[0])[None] for pieces in zip(*adapter)]
    return (token_grad, *adapter_grads)


def solution(mesh):
    row = P(AXES, None)
    block = P(AXES, None, None)
    in_specs = (row,) * 4 + (block,) * 7 + (P(None, "rep"),) * 3
    out_specs = (row,) + (block,) * 4

    return jax.shard_map(local, mesh=mesh, in_specs=in_specs, out_specs=out_specs, check_vma=False)
```

```python
import functools

import jax
import jax.numpy as jnp
from jax import lax
from jax.experimental import pallas as pl
from jax.experimental.pallas import tpu as pltpu
from jax.sharding import PartitionSpec as P


AXES = ("ep", "rep")
F32 = jnp.float32
BF16 = jnp.bfloat16


def dot(left, right, left_dim, right_dim):
    return lax.dot_general(
        left, right, (((left_dim,), (right_dim,)), ((), ())), preferred_element_type=F32
    )


def cotangents(gate_pre, up_pre, d_hidden):
    sig = jax.nn.sigmoid(gate_pre)
    d_gate = (d_hidden * up_pre * sig * (1.0 + gate_pre * (1.0 - sig))).astype(BF16)
    d_up = (d_hidden * gate_pre * sig).astype(BF16)
    return d_gate, d_up


def params(mib=56):
    return pltpu.CompilerParams(vmem_limit_bytes=mib * 1024 * 1024)


def selection(info_refs, peers, cap, want_weights):
    count = len(info_refs)
    info = [ref[...] for ref in info_refs]
    tokens = info[0].shape[1]
    places = jnp.concatenate(
        [jnp.where(a[:peers] >= 0.0, a[:peers] + float(i * cap), -1.0) for i, a in enumerate(info)],
        axis=1,
    )
    row = lax.broadcasted_iota(jnp.int32, (count * cap, count * tokens), 0).astype(F32)
    hot = [(row == places[d : d + 1, :]).astype(F32) for d in range(peers)]
    scale = None
    if want_weights:
        weights = jnp.concatenate([a[peers : 2 * peers] for a in info], axis=1)
        scale = jnp.concatenate(
            [
                jnp.sum(hot[d] * weights[d : d + 1, :], axis=1, keepdims=True)
                for d in range(peers)
            ],
            axis=0,
        )
    return jnp.concatenate(hot, axis=0), scale


def tile_of(width):
    return next((tile for tile in (768, 1152) if width % tile == 0), width)


def pack_kernel(peers, cap, counts, scaled, *refs):
    count = len(counts)
    info_refs, block_refs, out_refs = refs[:count], list(refs[count:-peers]), refs[-peers:]
    step = pl.program_id(0)
    hot, scale = selection(info_refs, peers, cap, scaled)
    blocks = []
    for n in counts:
        pieces = [block_refs.pop(0)[...] for _ in range(n)]
        block = pieces[0]
        for c in range(1, n):
            block = jnp.where(step == c, pieces[c], block)
        blocks.append(block)
    picked = dot(hot.astype(BF16), jnp.concatenate(blocks, axis=0), 1, 0)
    if scaled:
        picked = picked * scale
    for d in range(peers):
        out_refs[d][...] = picked[d * count * cap : (d + 1) * count * cap].astype(BF16)


def pack(infos, blocks, width, peers, cap, scaled):
    count = len(infos)
    tokens = infos[0].shape[1]
    cut = [block for block in blocks if isinstance(block, list) and len(block) > 1]
    tile = cut[0][0].shape[1] if cut else tile_of(width)
    whole = pl.BlockSpec(infos[0].shape, lambda i: (0, 0))
    arrays, specs, counts = [], [], []
    for block in blocks:
        if isinstance(block, list) and len(block) > 1:
            arrays += block
            specs += [pl.BlockSpec((tokens, tile), lambda i: (0, 0))] * len(block)
            counts.append(len(block))
            continue
        array, start = block if isinstance(block, tuple) else (block[0], 0)
        arrays.append(array)
        specs.append(
            pl.BlockSpec((tokens, tile), functools.partial(lambda at, i: (0, i + at), start // tile))
        )
        counts.append(1)
    return pl.pallas_call(
        functools.partial(pack_kernel, peers, cap, tuple(counts), scaled),
        grid=(width // tile,),
        in_specs=[whole] * count + specs,
        out_specs=[pl.BlockSpec((count * cap, tile), lambda i: (0, i))] * peers,
        out_shape=[jax.ShapeDtypeStruct((count * cap, width), BF16)] * peers,
        compiler_params=params(),
        cost_estimate=pl.CostEstimate(
            flops=2 * peers * count * cap * count * tokens * width,
            bytes_accessed=2 * width * (peers * count * cap + count * tokens),
            transcendentals=0,
        ),
    )(*infos, *arrays)


def merge_kernel(peers, cap, count, *refs):
    info_refs, back_refs, out_refs = refs[:count], refs[count : count + peers], refs[count + peers :]
    tokens = info_refs[0].shape[1]
    hot, _ = selection(info_refs, peers, cap, False)
    spread = jnp.transpose(hot).astype(BF16)
    back = jnp.concatenate([ref[...].astype(F32) for ref in back_refs], axis=0).astype(BF16)
    total = dot(spread, back, 1, 0)
    for i in range(count):
        out_refs[i][...] = total[i * tokens : (i + 1) * tokens].astype(out_refs[i].dtype)


def merge(infos, back, peers, cap, kinds):
    count = len(infos)
    tokens = infos[0].shape[1]
    width = back[0].shape[1]
    tile = tile_of(width)
    whole = pl.BlockSpec(infos[0].shape, lambda i: (0, 0))
    return pl.pallas_call(
        functools.partial(merge_kernel, peers, cap, count),
        grid=(width // tile,),
        in_specs=[whole] * count + [pl.BlockSpec((count * cap, tile), lambda i: (0, i))] * peers,
        out_specs=[pl.BlockSpec((tokens, tile), lambda i: (0, i))] * count,
        out_shape=[jax.ShapeDtypeStruct((tokens, width), kind) for kind in kinds],
        compiler_params=params(),
        cost_estimate=pl.CostEstimate(
            flops=2 * peers * count * cap * count * tokens * width,
            bytes_accessed=2 * width * (peers * count * cap + count * tokens),
            transcendentals=0,
        ),
    )(*infos, *back)


def expert_kernel(peers, steps, pieces, *refs):
    refs = list(refs)

    def take(count):
        taken, refs[:count] = refs[:count], []
        return taken

    row_refs, grad_refs = ([take(peers) for _ in range(n)] for n in pieces[:2])
    gate_w, up_w, down_w, gate_in, gate_out, up_in, up_out = take(7)
    out_refs = [take(peers) for _ in range(pieces[2])]
    gate_in_grad, gate_out_grad, up_in_grad, up_out_grad = take(4)
    rows, grads, total, low, maps_in, back = refs
    step = pl.program_id(0)
    height = row_refs[0][0].shape[0]
    rank = gate_in.shape[0]

    def gather(target, groups):
        at = 0
        for group in groups:
            wide = group[0].shape[1]
            target[:, at : at + wide] = jnp.concatenate(
                [r[...].astype(F32) for r in group], axis=0
            ).astype(BF16)
            at += wide

    @pl.when(step == 0)
    def _():
        gather(rows, row_refs)
        gather(grads, grad_refs)
        maps_in[:rank] = gate_in[...]
        maps_in[rank:] = up_in[...]
        low[...] = dot(rows[...], maps_in[...], 1, 1).astype(BF16)
        back[...] = jnp.zeros_like(back)

    low_gate, low_up = low[:, :rank], low[:, rank:]
    gate_pre = dot(rows[...], gate_w[...], 1, 0) + dot(low_gate, gate_out[...], 1, 0)
    up_pre = dot(rows[...], up_w[...], 1, 0) + dot(low_up, up_out[...], 1, 0)
    d_hidden = dot(grads[...], down_w[...], 1, 1)
    d_gate, d_up = cotangents(gate_pre, up_pre, d_hidden)
    back[:, :rank] += dot(d_gate, gate_out[...], 1, 1)
    back[:, rank:] += dot(d_up, up_out[...], 1, 1)
    gate_out_grad[...] = dot(low_gate, d_gate, 0, 0)
    up_out_grad[...] = dot(low_up, d_up, 0, 0)
    part = dot(d_gate, gate_w[...], 1, 1) + dot(d_up, up_w[...], 1, 1)

    @pl.when(step == 0)
    def _():
        total[...] = part

    @pl.when(step > 0)
    def _():
        total[...] += part

    @pl.when(step == steps - 1)
    def _():
        low_back = back[...].astype(BF16)
        done = total[...] + dot(low_back, maps_in[...], 1, 0)
        at = 0
        for group in out_refs:
            wide = group[0].shape[1]
            for d in range(peers):
                group[d][...] = done[d * height : (d + 1) * height, at : at + wide].astype(BF16)
            at += wide
        in_grads = dot(low_back, rows[...], 0, 0)
        gate_in_grad[...] = in_grads[:rank]
        up_in_grad[...] = in_grads[rank:]


def expert(rows, grads, weights, out_widths):
    peers = len(rows[0])
    height = rows[0][0].shape[0]
    gate_w, _, _, gate_in, _, _, _ = weights
    width, hidden = gate_w.shape
    rank = gate_in.shape[0]
    tile = 512 if hidden % 512 == 0 else hidden
    steps = hidden // tile
    count = peers * height

    def block(wide):
        return pl.BlockSpec((height, wide), lambda i: (0, 0))

    inputs = [array for group in rows + grads for array in group]
    wide = pl.BlockSpec((width, tile), lambda i: (0, i))
    low_in = pl.BlockSpec((rank, width), lambda i: (0, 0))
    low_out = pl.BlockSpec((rank, tile), lambda i: (0, i))
    result = pl.pallas_call(
        functools.partial(expert_kernel, peers, steps, (len(rows), len(grads), len(out_widths))),
        grid=(steps,),
        in_specs=[block(array.shape[1]) for array in inputs]
        + [wide, wide, pl.BlockSpec((tile, width), lambda i: (i, 0)), low_in, low_out, low_in, low_out],
        out_specs=[block(w) for w in out_widths for _ in range(peers)]
        + [low_in, low_out, low_in, low_out],
        out_shape=[jax.ShapeDtypeStruct((height, w), BF16) for w in out_widths for _ in range(peers)]
        + [
            jax.ShapeDtypeStruct((rank, width), F32),
            jax.ShapeDtypeStruct((rank, hidden), F32),
            jax.ShapeDtypeStruct((rank, width), F32),
            jax.ShapeDtypeStruct((rank, hidden), F32),
        ],
        scratch_shapes=[
            pltpu.VMEM((count, width), BF16),
            pltpu.VMEM((count, width), BF16),
            pltpu.VMEM((count, width), F32),
            pltpu.VMEM((count, 2 * rank), BF16),
            pltpu.VMEM((2 * rank, width), BF16),
            pltpu.VMEM((count, 2 * rank), F32),
        ],
        compiler_params=params(60),
        cost_estimate=pl.CostEstimate(
            flops=10 * count * width * hidden,
            bytes_accessed=6 * width * (count + hidden),
            transcendentals=count * hidden,
        ),
    )(*inputs, *weights)
    outs = [result[i * peers : (i + 1) * peers] for i in range(len(out_widths))]
    return outs, result[-4:]


def finish(base, terms):
    def kernel(*refs):
        base_ref, out = refs[0], refs[-1]
        at = 1
        pieces = []
        for term in terms:
            start = 0
            for piece in term:
                pieces.append((start, start + piece.shape[1], refs[at]))
                start += piece.shape[1]
                at += 1
        edges = sorted({0} | {hi for _, hi, _ in pieces})
        for lo, hi in zip(edges, edges[1:]):
            value = base_ref[:, lo:hi]
            for start, stop, ref in pieces:
                if start <= lo and hi <= stop:
                    value = value + ref[:, lo - start : hi - start].astype(F32)
            out[:, lo:hi] = value.astype(BF16)

    flat = [piece for term in terms for piece in term]
    return pl.pallas_call(
        kernel,
        out_shape=jax.ShapeDtypeStruct(base.shape, BF16),
        compiler_params=params(),
        cost_estimate=pl.CostEstimate(
            flops=base.size * (len(terms) + 1),
            bytes_accessed=base.size * (6 + 2 * len(terms)),
            transcendentals=0,
        ),
        name="finish",
    )(base, *flat)


def shared_kernel(full, parts, quarters, *refs):
    place, rows, grads = refs[:3]
    refs = refs[3:]
    width = rows.shape[1]
    out, stack_ref = refs[-2:]

    def add(stack, first):
        gate_w, up_w = stack[:width], stack[width : 2 * width]
        gate_pre = dot(rows[...], gate_w, 1, 0)
        up_pre = dot(rows[...], up_w, 1, 0)
        d_hidden = dot(grads[...], stack[2 * width :], 1, 0)
        d_gate, d_up = cotangents(gate_pre, up_pre, d_hidden)
        part = dot(d_gate, gate_w, 1, 1) + dot(d_up, up_w, 1, 1)
        if first:
            out[...] = part
        else:
            out[...] += part

    for i in range(full):
        add(refs[i], i == 0)
    for i in range(parts):
        for j in range(quarters):
            piece = refs[full + i * quarters + j]
            size = piece.shape[0]
            at = pl.multiple_of(jnp.bitwise_xor(place[0], j) * size, size)
            stack_ref[pl.ds(at, size), :] = piece[...]
        add(stack_ref, False)


def shared(place, rows, grads, whole_stacks, cut_stacks):
    full, parts, quarters = len(whole_stacks), len(cut_stacks), len(cut_stacks[0])
    tall, hidden = whole_stacks[0].shape
    count, width = rows.shape
    slices = full + parts
    vmem = pl.BlockSpec(memory_space=pltpu.VMEM)
    flat = whole_stacks + [piece for stack in cut_stacks for piece in stack]
    return pl.pallas_call(
        functools.partial(shared_kernel, full, parts, quarters),
        in_specs=[pl.BlockSpec(memory_space=pltpu.SMEM)] + [vmem] * (2 + len(flat)),
        out_shape=jax.ShapeDtypeStruct((count, width), F32),
        scratch_shapes=[pltpu.VMEM((tall, hidden), BF16)],
        compiler_params=params(),
        cost_estimate=pl.CostEstimate(
            flops=10 * count * width * hidden * slices,
            bytes_accessed=6 * width * hidden * slices,
            transcendentals=count * hidden * slices,
        ),
        name="shared",
    )(place, rows, grads, *flat)


def halvings(count):
    bits = []
    while count > 1:
        count //= 2
        bits.append(count)
    return bits


def plane_groups(planes):
    return [list(range(0, planes, 2)), list(range(1, planes, 2))]


def widths(width, pieces):
    return [width // pieces] * pieces if width % (128 * pieces) == 0 else [width]


IN_PIECES = 2
OUT_PIECES = 2


def local(
    tokens,
    output_grad,
    chosen_experts,
    route_weights,
    gate_weight,
    up_weight,
    down_weight,
    gate_adapter_in,
    gate_adapter_out,
    up_adapter_in,
    up_adapter_out,
    shared_gate,
    shared_up,
    shared_down,
):
    rep_count = lax.axis_size("rep")
    owners = lax.axis_size("ep") * rep_count
    peers = 2 * rep_count
    planes = owners // peers
    token_rows, model_width = tokens.shape
    pick_count = chosen_experts.shape[1]
    cap = token_rows * pick_count * 9 // (8 * owners)
    me = lax.axis_index(AXES)

    def swap(array, plane_step, peer_step):
        step = plane_step * peers + peer_step
        if step == 0:
            return array
        return lax.ppermute(array, AXES, [(i, i ^ step) for i in range(owners)])

    ids = me ^ lax.broadcasted_iota(jnp.int32, (owners, 1, 1), 0)
    named = chosen_experts.T[None] == ids
    weight = jnp.sum(jnp.where(named, route_weights.T[None], 0.0), axis=1)
    picked = jnp.any(named, axis=1)
    earlier = (
        lax.broadcasted_iota(jnp.int32, (token_rows, token_rows), 0)
        < lax.broadcasted_iota(jnp.int32, (token_rows, token_rows), 1)
    ).astype(BF16)
    ahead = jnp.dot(picked.astype(BF16), earlier, preferred_element_type=F32)
    place = jnp.where(picked, ahead, -1.0)
    info = jnp.concatenate(
        [place.reshape(planes, peers, token_rows), weight.reshape(planes, peers, token_rows)], axis=1
    )

    groups = plane_groups(planes)
    infos = {p: swap(info[p], p, 0) for p in range(planes)}
    every = [model_width]
    in_widths = widths(model_width, IN_PIECES)
    out_widths = widths(model_width, OUT_PIECES)

    weights = (
        gate_weight[0],
        up_weight[0],
        down_weight[0],
        gate_adapter_in[0],
        gate_adapter_out[0],
        up_adapter_in[0],
        up_adapter_out[0],
    )
    far, *rest = halvings(rep_count)
    place = (me // rep_count) % 4
    stack = jnp.concatenate([shared_gate, shared_up, shared_down], axis=0)
    quarter = stack.shape[0] // 4
    cut = [swap(lax.dynamic_slice_in_dim(stack, place * quarter, quarter), 0, far)]
    cut = cut + [swap(cut[0], 0, rep_count)]
    cut = cut + [swap(piece, 1, 0) for piece in cut]
    whole_stacks, cut_stacks = [stack], [cut]
    for bit in rest:
        whole_stacks = whole_stacks + [swap(s, 0, bit) for s in whole_stacks]
        cut_stacks = cut_stacks + [
            [swap(piece, 0, bit) for piece in pieces]
            for pieces in cut_stacks
        ]

    def blocks_of(array, sizes):
        held = {1: [swap(array, 1, 0)]}
        for p in groups[0]:
            pieces = []
            for c, size in enumerate(sizes):
                start = sum(sizes[:c])
                if p == 0:
                    pieces.append((array, start))
                    continue
                piece = array if len(sizes) == 1 else array[:, start : start + size]
                pieces.append(swap(piece, p, 0))
                held.setdefault(p + 1, []).append(swap(pieces[-1], 1, 0))
            held[p] = pieces
        return held

    def fan_out(arrays):
        return [swap(arrays[d], 0, d) for d in range(peers)]

    token_blocks = blocks_of(tokens, in_widths)
    grad_blocks = blocks_of(output_grad, every)
    terms = []
    adapter = []
    for g, group in enumerate(groups):
        seen = [infos[p] for p in group]
        sizes, out_sizes = (in_widths, every) if g == 0 else (every, out_widths)
        rows = []
        for c, size in enumerate(sizes):
            blocks = [token_blocks[p] if g else token_blocks[p][c] for p in group]
            blocks = [b if isinstance(b, (list, tuple)) else (b, 0) for b in blocks]
            packed = pack(seen, blocks, size, peers, cap, False)
            rows.append(fan_out(packed))
        blocks = [grad_blocks[p] if g else grad_blocks[p][0] for p in group]
        blocks = [b if isinstance(b, (list, tuple)) else (b, 0) for b in blocks]
        packed = pack(seen, blocks, model_width, peers, cap, True)
        grads = [fan_out(packed)]
        outs, grads_of_maps = expert(rows, grads, weights, out_sizes)
        adapter.append(grads_of_maps)
        found = {p: [] for p in group}
        for out in outs:
            back = fan_out(out)
            kinds = [F32 if p == 0 else BF16 for p in group]
            merged = merge(seen, back, peers, cap, kinds)
            for p, part in zip(group, merged):
                found[p].append(swap(part, p, 0))
        terms += list(found.values())
    base = shared(place.reshape(1), tokens, output_grad, whole_stacks, cut_stacks)
    token_grad = finish(base, terms)
    adapter_grads = [sum(pieces[1:], pieces[0])[None] for pieces in zip(*adapter)]
    return (token_grad, *adapter_grads)


def solution(mesh):
    row = P(AXES, None)
    block = P(AXES, None, None)
    in_specs = (row,) * 4 + (block,) * 7 + (P(None, "rep"),) * 3
    out_specs = (row,) + (block,) * 4

    return jax.shard_map(local, mesh=mesh, in_specs=in_specs, out_specs=out_specs, check_vma=False)
```
